32 devices in a mesh: req: 8 (over z, core), blk: 4 (over y, x).
Axes of the slice: x: 2, y: 2, z: 4, core: 2. Of those that a mesh axis runs over, the one named last changes fastest.
Arguments:
- draft_node_queries: bfloat16 [256, 4096], P(('req', 'blk')), parts along dimension 0, may hold values from -6 to 6, as said below
- draft_node_keys: bfloat16 [256, 512], P(('req', 'blk')), parts along dimension 0, may hold values from -6 to 6
- draft_node_values: bfloat16 [256, 512], P(('req', 'blk')), parts along dimension 0, may hold values from -6 to 6
- paged_key_cache: bfloat16 [16384, 512], P(('req', 'blk')), parts along dimension 0, may hold values from -6 to 6
- paged_value_cache: bfloat16 [16384, 512], P(('req', 'blk')), parts along dimension 0, may hold values from -6 to 6
- context_length: int32 [8], P('req'), parts along dimension 0, may hold values from 1024 to 2048
- parents: int32 [256], P('req'), parts along dimension 0, may hold values from 0 to 31, as said below
- accepted_path: int32 [64], P('req'), parts along dimension 0, may hold values from 0 to 31, as said below
- out_weight: bfloat16 [2880, 4096], P('blk'), may hold values from -0.09375 to 0.09375
Outputs:
- tree_attention: bfloat16 [256, 4096], P(('req', 'blk')), parts along dimension 0
- path_output: bfloat16 [64, 2880], P('req', 'blk'), parts along dimension 0
The draws below stay inside these ranges and needn't reach their ends.
There are 8 independent parts, one for each index of `req`. The reference program is written for one: setup_inputs(seed, part) draws one part's arguments, and reference() takes and returns one part's arrays. A program takes and returns all parts, laid end to end along the dimension named above; an argument that names none is the same for every part. Nothing has to cross between parts.
Inputs may be any that keep to these rules, and one draw needn't show every extreme that they name: `draft_node_queries`: query entries lie within the range. parents[0] = 0 marks the root; for i >= 1, parents[i] is one of the nodes i - 4 to i - 1 (and at least 0). `accepted_path`: distinct nodes; each entry after the first is a child of the one before it.
All inputs are finite; a program needn't handle non-finite values.
Results may differ from the reference program's by a relative error of at most 0.0095.
Values may be sent and summed in bfloat16 or wider, within the bound.
A program may use at most 64 MiB of HBM per device.

```python
import jax
import jax.numpy as jnp
from jax import lax

D = 2880
QUERY_HEADS = 64
KEY_VALUE_HEADS = 8
HEAD_WIDTH = 64
TREE_NODES = 32
PATH = 8
CACHED_LENGTH = 2048


def tree_links(key):
    window = TREE_NODES // 8
    indices = jnp.arange(TREE_NODES, dtype=jnp.int32)
    lowest = jnp.maximum(indices - window, 0)
    spread = jnp.maximum(indices - lowest, 1)
    offsets = jax.random.randint(jax.random.fold_in(key, 31), (TREE_NODES,), 0, 1 << 20, dtype=jnp.int32)
    linked = lowest + offsets % spread
    return jnp.where(indices == 0, 0, linked).astype(jnp.int32)


def draw_parents(key, part):
    return tree_links(key)


def draw_accepted_path(key, part):
    linked = tree_links(key)
    window = TREE_NODES // 8
    leaf_node = TREE_NODES - 1 - jax.random.randint(jax.random.fold_in(key, 32), (), 0, window, dtype=jnp.int32)
    walked = [leaf_node]
    for stepper in range(PATH - 1):
        walked.append(linked[walked[-1]])
    return jnp.stack(walked[::-1]).astype(jnp.int32)


def draw_draft_node_queries(key, part):
    base_offset = jax.random.normal(jax.random.fold_in(key, 11), (TREE_NODES, QUERY_HEADS * HEAD_WIDTH), jnp.float32)
    return jnp.clip(2.5 * base_offset, -6.0, 6.0).astype(jnp.bfloat16)


def draw_paged_key_cache(key, part):
    base_offset = jax.random.normal(jax.random.fold_in(key, 22), (CACHED_LENGTH, KEY_VALUE_HEADS * HEAD_WIDTH), jnp.float32)
    return jnp.clip(base_offset, -6.0, 6.0).astype(jnp.bfloat16)


def block_levels(key, shape, shards, smallest, high):
    def one(axis_at, shards_of):
        steps = jax.random.uniform(jax.random.fold_in(jax.random.fold_in(key, 6), axis_at), (shards_of,), jnp.float32, smallest / len(shards), high / len(shards))
        return jnp.repeat(jnp.exp(steps), shape[axis_at] // shards_of).reshape((-1,) + (1,) * (len(shape) - axis_at - 1))

    level = one(*shards[0])
    for cut in shards[1:]:
        level = level * one(*cut)
    return level


def bell_draw(stream_key, dims, scale, reach, split=(), kind=jnp.bfloat16):
    array = jax.random.normal(stream_key, dims, jnp.float32) * scale
    if len(split) > 0:
        array = block_levels(stream_key, dims, split, -0.22, 0.18) * array
    return jnp.clip(array, min=-reach, max=reach).astype(kind)


def setup_inputs(seed: int = 0, part: int = 0) -> dict:
    key_of = jax.random.split(jax.random.key(seed), 10)
    part_splits = jax.random.split(jax.random.fold_in(key_of[9], part), 10)
    draft_node_queries = draw_draft_node_queries(jax.random.fold_in(jax.random.fold_in(key_of[9], part), 71), part)
    draft_node_keys = bell_draw(part_splits[1], (TREE_NODES, KEY_VALUE_HEADS * HEAD_WIDTH), 1.0, 6.0, ((0, 4),))
    draft_node_values = bell_draw(part_splits[2], (TREE_NODES, KEY_VALUE_HEADS * HEAD_WIDTH), 1.0, 6.0, ((0, 4),))
    paged_key_cache = draw_paged_key_cache(jax.random.fold_in(jax.random.fold_in(key_of[9], part), 71), part)
    paged_value_cache = bell_draw(part_splits[4], (CACHED_LENGTH, KEY_VALUE_HEADS * HEAD_WIDTH), 1.0, 6.0, ((0, 4),))
    context_length = jax.random.randint(part_splits[5], (1,), CACHED_LENGTH // 2, CACHED_LENGTH + 1).astype(jnp.int32)
    parents = draw_parents(jax.random.fold_in(jax.random.fold_in(key_of[9], part), 71), part)
    accepted_path = draw_accepted_path(jax.random.fold_in(jax.random.fold_in(key_of[9], part), 71), part)
    out_weight = bell_draw(key_of[8], (D, QUERY_HEADS * HEAD_WIDTH), (QUERY_HEADS * HEAD_WIDTH) ** -0.5, 0.09375, ((0, 4),))
    return dict(draft_node_queries=draft_node_queries, draft_node_keys=draft_node_keys, draft_node_values=draft_node_values, paged_key_cache=paged_key_cache, paged_value_cache=paged_value_cache, context_length=context_length, parents=parents, accepted_path=accepted_path, out_weight=out_weight)


score_after_mask = -1.0e30


def ancestors(parents):
    indices = jnp.arange(TREE_NODES, dtype=jnp.int32)
    linked = (parents[:, None] == indices[None, :]) & (indices[:, None] > 0)
    ancestry = jnp.minimum(jnp.eye(TREE_NODES, dtype=jnp.float32) + linked.astype(jnp.float32), 1.0)
    for squaring in range(7):
        ancestry = jnp.minimum(jnp.dot(ancestry, ancestry, precision=lax.Precision.HIGHEST), 1.0)
    return ancestry > 0.5


def reference(draft_node_queries, draft_node_keys, draft_node_values, paged_key_cache, paged_value_cache, context_length, parents, accepted_path, out_weight):
    query_group_width = QUERY_HEADS // KEY_VALUE_HEADS
    inverse_root_scale = HEAD_WIDTH ** -0.5
    rows_per_block = min(512, CACHED_LENGTH)
    block_table = CACHED_LENGTH // rows_per_block
    length = context_length[0]
    grouped_queries = draft_node_queries.astype(jnp.float32).reshape(TREE_NODES, KEY_VALUE_HEADS, query_group_width, HEAD_WIDTH)
    gathered_key_blocks = paged_key_cache.reshape(block_table, rows_per_block, KEY_VALUE_HEADS, HEAD_WIDTH)
    gathered_value_blocks = paged_value_cache.reshape(block_table, rows_per_block, KEY_VALUE_HEADS, HEAD_WIDTH)
    starts = rows_per_block * jnp.arange(block_table, dtype=jnp.int32)
    ancestry = ancestors(parents)

    def block_scores(gathered_key_block, start_pos):
        scores = jnp.einsum("mrjz,xrz->mrjx", grouped_queries, gathered_key_block.astype(jnp.float32)) * inverse_root_scale
        usable = (start_pos + jnp.arange(rows_per_block, dtype=jnp.int32)) < length
        return jnp.where(usable, scores, score_after_mask), usable

    draft_node_scores = jnp.einsum("mrjz,xrz->mrjx", grouped_queries, draft_node_keys.astype(jnp.float32).reshape(TREE_NODES, KEY_VALUE_HEADS, HEAD_WIDTH)) * inverse_root_scale
    tree_usable = ancestry[:, None, None, :]
    draft_node_scores = jnp.where(tree_usable, draft_node_scores, score_after_mask)

    def max_step(maxima, pieces):
        scores, usable = block_scores(pieces[0], pieces[1])
        return jnp.maximum(maxima, jnp.max(scores, axis=-1)), None

    maxima, unused = lax.scan(max_step, jnp.max(draft_node_scores, axis=-1), (gathered_key_blocks, starts))

    def sum_step(state, pieces):
        totals, weighted = state
        scores, usable = block_scores(pieces[0], pieces[1])
        probs = jnp.where(usable, jnp.exp(scores - maxima[..., None]), 0.0)
        rounded = probs.astype(jnp.bfloat16).astype(jnp.float32)
        weighted = weighted + jnp.einsum("zvle,evt->zvlt", rounded, pieces[2].astype(jnp.float32))
        return (totals + jnp.sum(probs, axis=-1), weighted), None

    tree_probs = jnp.where(tree_usable, jnp.exp(draft_node_scores - maxima[..., None]), 0.0)
    draft_rounded_scores = tree_probs.astype(jnp.bfloat16).astype(jnp.float32)
    initial_weighted_sum = jnp.einsum("zvle,evt->zvlt", draft_rounded_scores, draft_node_values.astype(jnp.float32).reshape(TREE_NODES, KEY_VALUE_HEADS, HEAD_WIDTH))
    (totals, weighted), unused = lax.scan(sum_step, (jnp.sum(tree_probs, axis=-1), initial_weighted_sum), (gathered_key_blocks, starts, gathered_value_blocks))
    attention = (weighted / totals[..., None]).astype(jnp.bfloat16).reshape(TREE_NODES, QUERY_HEADS * HEAD_WIDTH)
    picker = (accepted_path[:, None] == jnp.arange(TREE_NODES, dtype=jnp.int32)[None, :]).astype(jnp.bfloat16)
    path_rows = jnp.dot(picker, attention, preferred_element_type=jnp.float32).astype(jnp.bfloat16)
    path_output = lax.dot_general(path_rows, out_weight, (((1,), (1,)), ((), ())), preferred_element_type=jnp.float32).astype(jnp.bfloat16)
    return attention, path_output
```

```python
import functools
import math

import jax
import jax.numpy as jnp
from jax import lax
from jax.experimental import pallas as pl
from jax.experimental.pallas import tpu as pltpu
from jax.sharding import PartitionSpec as P

QUERY_HEADS = 64
KEY_VALUE_HEADS = 8
HEAD_WIDTH = 64
GROUP = QUERY_HEADS // KEY_VALUE_HEADS
LANES = 128
HALF = LANES // 2
SPAN = GROUP * HEAD_WIDTH
PAIRS = SPAN // LANES
CHUNKS = KEY_VALUE_HEADS // 2
CHUNK = 2 * SPAN
ROWS = LANES // (2 * GROUP)
DEPTH = HEAD_WIDTH + 8
TILE = 16
UNIT = 256
LAG = 1
EXCLUDED = -1e30
FLOOR = -1e20
SCALE = HEAD_WIDTH ** (-0.5)
EXPONENT = SCALE * math.log2(math.e)
NT = (((1,), (1,)), ((), ()))
MESH = pl.DeviceIdType.MESH


def partner(me, k, n):
    if n & (n - 1):
        return lax.rem(me + k, n)
    other = me
    bit = 1
    while bit < n:
        if k & bit:
            other = other + bit - 2 * bit * ((me // bit) % 2)
        bit *= 2
    return other


def split(value):
    first = value.astype(jnp.bfloat16).astype(jnp.float32)
    rest = value - first
    second = rest.astype(jnp.bfloat16).astype(jnp.float32)
    return [first, second, rest - second]


def fold(top, total):
    row = lax.broadcasted_iota(jnp.int32, total.shape, 0)
    stat = jnp.zeros_like(total)
    for at, term in enumerate(split(jnp.broadcast_to(top, total.shape)) + split(total)):
        stat = jnp.where(row == at, term, stat)
    return stat


def merge(parts):
    stats = [part[HEAD_WIDTH:] for part in parts]
    tops = [stat[0:1] + stat[1:2] + stat[2:3] for stat in stats]
    totals = [stat[3:4] + stat[4:5] + stat[5:6] for stat in stats]
    top = functools.reduce(jnp.maximum, tops)
    shares = [jnp.exp2((each - top) * EXPONENT) for each in tops]
    total = functools.reduce(jnp.add, [share * each for share, each in zip(shares, totals)])
    merged = functools.reduce(
        jnp.add, [part[:HEAD_WIDTH] * (share / total) for share, part in zip(shares, parts)]
    )
    turned = jnp.concatenate([merged, pltpu.roll(merged, LANES - ROWS, 1)], axis=0).T
    return jnp.concatenate(
        [turned[2 * ROWS * pair : 2 * ROWS * pair + ROWS] for pair in range(2 * PAIRS)], axis=1
    ).astype(jnp.bfloat16)


def kernel(
    n, own, nodes,
    length_hbm, parents_hbm, path_hbm, q_ref, k_ref, v_ref, kc_ref, vc_ref, w_ref,
    att_ref, out_ref,
    length_ref, parents_ref, path_ref, kown, vown,
    qbuf, kbuf, vbuf, wbuf, keys, values, sbuf, rbuf, psend, pbuf, picks, acc,
    load_sem, q_recv, r_recv, p_recv, sends,
):
    me = lax.axis_index("blk")
    rows = q_ref.shape[0]
    wide = n * rows
    cached = kc_ref.shape[0]
    picked = path_hbm.shape[0]
    peers = [partner(me, k, n) for k in range(n - 1, 0, -1)]

    load_q = pltpu.make_async_copy(q_ref, qbuf.at[me], load_sem.at[0])
    load_q.start()
    small_loads = [
        pltpu.make_async_copy(src, dst, load_sem.at[4 + i])
        for i, (src, dst) in enumerate((
            (parents_hbm, parents_ref), (length_hbm, length_ref), (path_hbm, path_ref),
            (k_ref, kown), (v_ref, vown),
        ))
    ]
    for copy in small_loads:
        copy.start()
    load_k = pltpu.make_async_copy(kc_ref, kbuf, load_sem.at[1])
    load_v = pltpu.make_async_copy(vc_ref, vbuf, load_sem.at[2])
    load_w = pltpu.make_async_copy(w_ref, wbuf, load_sem.at[3])
    load_k.start()
    load_v.start()

    barrier = pltpu.get_barrier_semaphore()
    for peer in peers:
        pl.semaphore_signal(barrier, inc=1, device_id={"blk": peer}, device_id_type=MESH)
    pl.semaphore_wait(barrier, n - 1)

    def q_copy(c, peer):
        columns = pl.ds(c * CHUNK, CHUNK)
        return pltpu.make_async_remote_copy(
            src_ref=qbuf.at[me, :, columns], dst_ref=qbuf.at[me, :, columns],
            send_sem=sends.at[0], recv_sem=q_recv.at[c],
            device_id={"blk": peer}, device_id_type=MESH,
        )

    def r_copy(c, peer):
        return pltpu.make_async_remote_copy(
            src_ref=sbuf.at[c, peer], dst_ref=rbuf.at[c, me],
            send_sem=sends.at[1], recv_sem=r_recv.at[c],
            device_id={"blk": peer}, device_id_type=MESH,
        )

    def p_copy(c, peer):
        return pltpu.make_async_remote_copy(
            src_ref=psend.at[c], dst_ref=pbuf.at[c, me],
            send_sem=sends.at[2], recv_sem=p_recv.at[c],
            device_id={"blk": peer}, device_id_type=MESH,
        )

    def arrived(block, sem):
        pltpu.make_async_copy(block, block, sem).wait()

    others = pl.ds(0, n - 1)
    load_q.wait()
    for c in range(CHUNKS):
        for peer in peers:
            q_copy(c, peer).start()
    load_w.start()

    for copy in small_loads:
        copy.wait()

    up = lax.broadcasted_iota(jnp.int32, (wide, wide), 0)
    down = lax.broadcasted_iota(jnp.int32, (wide, wide), 1)
    up_node = up // rows * own + up % rows
    links = jnp.where(up == down, 1.0, 0.0)
    for i in range(1, nodes):
        at = i // own * rows + i % own
        links = jnp.where((down == at) & (up_node == parents_ref[i]) & (up % rows < own), 1.0, links)
    for squaring in range(max(1, math.ceil(math.log2(nodes)))):
        half = links.astype(jnp.bfloat16)
        links = jnp.minimum(jnp.dot(half, half, preferred_element_type=jnp.float32), 1.0)
    source = lax.broadcasted_iota(jnp.int32, (wide, LANES), 0)
    lane = lax.broadcasted_iota(jnp.int32, (wide, LANES), 1)
    spare = lane % HALF
    mine = jnp.where((source == me * rows + spare - 1) & (spare >= 1) & (spare <= own), 1.0, 0.0)
    related = lax.dot_general(
        links.astype(jnp.bfloat16), mine.astype(jnp.bfloat16), (((0,), (0,)), ((), ())),
        preferred_element_type=jnp.float32,
    )
    marks = jnp.where(
        spare == 0, 1.0,
        jnp.where((spare <= own) & (related < 0.5), EXCLUDED, 0.0),
    )

    size = n * HALF
    at = lax.broadcasted_iota(jnp.int32, (2 * size, LANES), 0)
    goal = lax.broadcasted_iota(jnp.int32, (2 * size, LANES), 1)
    spot_node = at % size // HALF * own + at % ROWS
    wanted = jnp.full((2 * size, LANES), -1, jnp.int32)
    for k in range(picked):
        wanted = jnp.where(goal % ROWS == k, path_ref[k], wanted)
    same = (at // size == goal // HALF) & (at % HALF // ROWS == goal % HALF // ROWS)
    picks[...] = jnp.where(
        same & (wanted == spot_node) & (at % ROWS < own), 1.0, 0.0
    ).astype(jnp.bfloat16)

    place = lax.broadcasted_iota(jnp.int32, (cached, LANES), 0) + me * cached
    column = lax.broadcasted_iota(jnp.int32, (cached, LANES), 1)
    spent = jnp.where((column % HALF == 0) & (place >= length_ref[0]), EXCLUDED, 0.0)
    node = lax.broadcasted_iota(jnp.int32, (TILE, LANES), 0)
    node_lane = lax.broadcasted_iota(jnp.int32, (TILE, LANES), 1)
    node_spare = node_lane % HALF
    tags = jnp.where(
        node < own, jnp.where(node_spare == node + 1, 1.0, 0.0),
        jnp.where(node_spare == 0, EXCLUDED, 0.0),
    )
    blank = jnp.zeros((LANES - rows, LANES), jnp.float32)
    load_k.wait()
    for h in range(KEY_VALUE_HEADS):
        columns = slice(h // 2 * LANES, (h // 2 + 1) * LANES)
        held = (column < HALF) if h % 2 == 0 else (column >= HALF)
        node_held = (node_lane < HALF) if h % 2 == 0 else (node_lane >= HALF)
        keys[h, pl.ds(0, cached)] = jnp.where(
            held, kbuf[:, columns].astype(jnp.float32), spent
        ).astype(jnp.bfloat16)
        fresh = jnp.concatenate([kown[:, columns].astype(jnp.float32), blank], axis=0)
        keys[h, pl.ds(cached, TILE)] = jnp.where(node_held, fresh[:TILE], tags).astype(jnp.bfloat16)
    load_v.wait()
    for c in range(CHUNKS):
        columns = slice(c * LANES, (c + 1) * LANES)
        fresh = jnp.concatenate([vown[:, columns].astype(jnp.float32), blank], axis=0)
        turned = vbuf[:, columns].astype(jnp.float32).T.astype(jnp.bfloat16)
        fresh = fresh.T.astype(jnp.bfloat16)
        for side in range(2):
            half = slice(side * HALF, (side + 1) * HALF)
            values[2 * c + side, pl.ds(0, HALF), pl.ds(0, cached)] = turned[half]
            values[2 * c + side, pl.ds(0, HALF), pl.ds(cached, LANES)] = fresh[half]
            values[2 * c + side, pl.ds(HALF, 16)] = jnp.ones((16, cached + LANES), jnp.bfloat16)

    low = lax.broadcasted_iota(jnp.int32, (rows, LANES), 1) < HALF
    deep_low = lax.broadcasted_iota(jnp.int32, (DEPTH, LANES), 1) < HALF
    for c in range(CHUNKS):
        arrived(qbuf.at[others, :, pl.ds(c * CHUNK, CHUNK)], q_recv.at[c])
        q = qbuf[:, :, c * CHUNK : (c + 1) * CHUNK].astype(jnp.float32)
        asked = []
        for side in range(2):
            keep = low if side == 0 else jnp.logical_not(low)
            stacked = []
            for d in range(n):
                extra = marks[d * rows : (d + 1) * rows]
                for pair in range(PAIRS):
                    start = side * SPAN + pair * LANES
                    tile = q[d, :, start : start + LANES]
                    turned = pltpu.roll(tile, HALF, 1)
                    even, odd = (tile, turned) if side == 0 else (turned, tile)
                    stacked.append(jnp.where(keep, even, extra))
                    stacked.append(jnp.where(keep, odd, extra))
            queries = jnp.concatenate(stacked, axis=0).astype(jnp.bfloat16)
            asked += [
                (2 * c + side, queries[start : start + UNIT]) for start in range(0, size, UNIT)
            ]

        def score(h, queries):
            return lax.dot_general(keys[h], queries, NT, preferred_element_type=jnp.float32)

        def weigh(h, scores):
            top = jnp.maximum(jnp.max(scores, axis=0, keepdims=True), FLOOR)
            weights = jnp.exp2((scores - top) * EXPONENT).astype(jnp.bfloat16)
            weighted = jnp.dot(
                values[h, :, pl.ds(0, cached)], weights[:cached], preferred_element_type=jnp.float32
            ) + jnp.dot(
                values[h, :, pl.ds(cached, TILE)], weights[cached:],
                preferred_element_type=jnp.float32,
            )
            return jnp.concatenate([weighted[:HALF], fold(top, weighted[HALF:DEPTH])], axis=0)

        done, waiting = [], []
        for h, queries in asked:
            waiting.append((h, score(h, queries)))
            if len(waiting) > LAG:
                done.append(weigh(*waiting.pop(0)))
        done += [weigh(*each) for each in waiting]
        per = len(done) // 2
        full = [jnp.concatenate(done[side * per : (side + 1) * per], axis=1) for side in range(2)]
        for d in range(n):
            block = slice(d // 2 * LANES, (d // 2 + 1) * LANES)
            left, right = full[0][:, block], full[1][:, block]
            if d % 2 == 0:
                right = pltpu.roll(right, HALF, 1)
            else:
                left = pltpu.roll(left, HALF, 1)
            sbuf[c, d] = jnp.where(deep_low, left, right).astype(jnp.bfloat16)
        for peer in peers:
            r_copy(c, peer).start()
        psend[c] = jnp.dot(
            jnp.concatenate(full, axis=1).astype(jnp.bfloat16), picks[...],
            preferred_element_type=jnp.float32,
        ).astype(jnp.bfloat16)
        for peer in peers:
            p_copy(c, peer).start()

    load_w.wait()
    acc[...] = jnp.zeros_like(acc)
    for c in range(CHUNKS):
        columns = pl.ds(c * CHUNK, CHUNK)
        arrived(rbuf.at[c, others], r_recv.at[c])
        arrived(pbuf.at[c, others], p_recv.at[c])
        parts = [sbuf[c, me]] + [rbuf[c, peer] for peer in peers]
        att_ref[:, columns] = merge([part.astype(jnp.float32) for part in parts])
        parts = [psend[c]] + [pbuf[c, peer] for peer in peers]
        acc[...] += lax.dot_general(
            merge([part.astype(jnp.float32) for part in parts]), wbuf[:, columns], NT,
            preferred_element_type=jnp.float32,
        )
    out_ref[...] = acc[...].astype(jnp.bfloat16)

    arrived(qbuf.at[others], sends.at[0])
    arrived(rbuf.at[:, others], sends.at[1])
    arrived(pbuf.at[:, others], sends.at[2])


def write_out(att_ref, out_ref, att_hbm, out_hbm, sems):
    copies = [
        pltpu.make_async_copy(att_ref, att_hbm, sems.at[0]),
        pltpu.make_async_copy(out_ref, out_hbm, sems.at[1]),
    ]
    for copy in copies:
        copy.start()
    for copy in copies:
        copy.wait()


def local(
    n,
    draft_node_queries,
    draft_node_keys,
    draft_node_values,
    paged_key_cache,
    paged_value_cache,
    context_length,
    parents,
    accepted_path,
    out_weight,
):
    own = draft_node_queries.shape[0]
    rows = -(-own // 8) * 8
    if rows != own:
        pad = ((0, rows - own), (0, 0))
        draft_node_queries = jnp.pad(draft_node_queries, pad)
        draft_node_keys = jnp.pad(draft_node_keys, pad)
        draft_node_values = jnp.pad(draft_node_values, pad)
    cached, cache_width = paged_key_cache.shape
    picked = accepted_path.shape[0]
    q_width = QUERY_HEADS * HEAD_WIDTH
    vmem = pl.BlockSpec(memory_space=pltpu.VMEM)
    anywhere = pl.BlockSpec(memory_space=pltpu.HBM)
    shapes = (
        jax.ShapeDtypeStruct((rows, q_width), jnp.bfloat16),
        jax.ShapeDtypeStruct((picked, out_weight.shape[0]), jnp.bfloat16),
    )
    held = pl.pallas_call(
        functools.partial(kernel, n, own, parents.shape[0]),
        out_shape=tuple(pltpu.VMEM(shape.shape, shape.dtype) for shape in shapes),
        in_specs=[anywhere] * 9,
        out_specs=(vmem, vmem),
        scratch_shapes=[
            pltpu.SMEM(context_length.shape, jnp.int32),
            pltpu.SMEM(parents.shape, jnp.int32),
            pltpu.SMEM(accepted_path.shape, jnp.int32),
            pltpu.VMEM((rows, cache_width), jnp.bfloat16),
            pltpu.VMEM((rows, cache_width), jnp.bfloat16),
            pltpu.VMEM((n, rows, q_width), jnp.bfloat16),
            pltpu.VMEM((cached, cache_width), jnp.bfloat16),
            pltpu.VMEM((cached, cache_width), jnp.bfloat16),
            pltpu.VMEM(out_weight.shape, jnp.bfloat16),
            pltpu.VMEM((KEY_VALUE_HEADS, cached + TILE, LANES), jnp.bfloat16),
            pltpu.VMEM((KEY_VALUE_HEADS, HALF + 16, cached + LANES), jnp.bfloat16),
            pltpu.VMEM((CHUNKS, n, DEPTH, LANES), jnp.bfloat16),
            pltpu.VMEM((CHUNKS, n, DEPTH, LANES), jnp.bfloat16),
            pltpu.VMEM((CHUNKS, DEPTH, LANES), jnp.bfloat16),
            pltpu.VMEM((CHUNKS, n, DEPTH, LANES), jnp.bfloat16),
            pltpu.VMEM((2 * n * HALF, LANES), jnp.bfloat16),
            pltpu.VMEM((picked, out_weight.shape[0]), jnp.float32),
            pltpu.SemaphoreType.DMA((9,)),
            pltpu.SemaphoreType.DMA((CHUNKS,)),
            pltpu.SemaphoreType.DMA((CHUNKS,)),
            pltpu.SemaphoreType.DMA((CHUNKS,)),
            pltpu.SemaphoreType.DMA((3,)),
        ],
        compiler_params=pltpu.CompilerParams(
            collective_id=0, has_side_effects=True, vmem_limit_bytes=56 * 1024 * 1024
        ),
        name="verify_tree",
    )(
        context_length, parents, accepted_path,
        draft_node_queries, draft_node_keys, draft_node_values,
        paged_key_cache, paged_value_cache, out_weight,
    )
    attention, path_output = pl.pallas_call(
        write_out,
        out_shape=shapes,
        in_specs=(vmem, vmem),
        out_specs=(anywhere, anywhere),
        scratch_shapes=[pltpu.SemaphoreType.DMA((2,))],
        compiler_params=pltpu.CompilerParams(vmem_limit_bytes=1024 * 1024),
        name="write_out",
    )(*held)
    return attention[:own], path_output


def solution(mesh):
    in_specs = (
        P(("req", "blk"), None),
        P(("req", "blk"), None),
        P(("req", "blk"), None),
        P(("req", "blk"), None),
        P(("req", "blk"), None),
        P("req"),
        P("req"),
        P("req"),
        P("blk", None),
    )
    out_specs = (P(("req", "blk"), None), P("req", "blk"))
    return jax.shard_map(
        functools.partial(local, mesh.shape["blk"]),
        mesh=mesh, in_specs=in_specs, out_specs=out_specs, check_vma=False,
    )
```

```python
import functools
import math

import jax
import jax.numpy as jnp
from jax import lax
from jax.experimental import pallas as pl
from jax.experimental.pallas import tpu as pltpu
from jax.sharding import PartitionSpec as P

QUERY_HEADS = 64
KEY_VALUE_HEADS = 8
HEAD_WIDTH = 64
GROUP = QUERY_HEADS // KEY_VALUE_HEADS
LANES = 128
HALF = LANES // 2
SPAN = GROUP * HEAD_WIDTH
PAIRS = SPAN // LANES
CHUNKS = KEY_VALUE_HEADS // 2
CHUNK = 2 * SPAN
ROWS = LANES // (2 * GROUP)
DEPTH = HEAD_WIDTH + 8
TILE = 16
UNIT = 256
LAG = 1
EXCLUDED = -1e30
FLOOR = -1e20
SCALE = HEAD_WIDTH ** (-0.5)
EXPONENT = SCALE * math.log2(math.e)
NT = (((1,), (1,)), ((), ()))
MESH = pl.DeviceIdType.MESH


def partner(me, k, n):
    if n & (n - 1):
        return lax.rem(me + k, n)
    other = me
    bit = 1
    while bit < n:
        if k & bit:
            other = other + bit - 2 * bit * ((me // bit) % 2)
        bit *= 2
    return other


def split(value):
    first = value.astype(jnp.bfloat16).astype(jnp.float32)
    rest = value - first
    second = rest.astype(jnp.bfloat16).astype(jnp.float32)
    return [first, second, rest - second]


def fold(top, total):
    row = lax.broadcasted_iota(jnp.int32, total.shape, 0)
    stat = jnp.zeros_like(total)
    for at, term in enumerate(split(jnp.broadcast_to(top, total.shape)) + split(total)):
        stat = jnp.where(row == at, term, stat)
    return stat


def merge(parts):
    stats = [part[HEAD_WIDTH:] for part in parts]
    tops = [stat[0:1] + stat[1:2] + stat[2:3] for stat in stats]
    totals = [stat[3:4] + stat[4:5] + stat[5:6] for stat in stats]
    top = functools.reduce(jnp.maximum, tops)
    shares = [jnp.exp2((each - top) * EXPONENT) for each in tops]
    total = functools.reduce(jnp.add, [share * each for share, each in zip(shares, totals)])
    merged = functools.reduce(
        jnp.add, [part[:HEAD_WIDTH] * (share / total) for share, part in zip(shares, parts)]
    )
    turned = jnp.concatenate([merged, pltpu.roll(merged, LANES - ROWS, 1)], axis=0).T
    return jnp.concatenate(
        [turned[2 * ROWS * pair : 2 * ROWS * pair + ROWS] for pair in range(2 * PAIRS)], axis=1
    ).astype(jnp.bfloat16)


def kernel(
    n, own, nodes,
    length_hbm, parents_hbm, path_hbm, q_ref, k_ref, v_ref, kc_ref, vc_ref, w_ref,
    att_ref, out_ref,
    length_ref, parents_ref, path_ref, kown, vown,
    qbuf, kbuf, vbuf, wbuf, keys, values, sbuf, rbuf, psend, pbuf, picks, acc,
    load_sem, q_recv, r_recv, p_recv, sends,
):
    me = lax.axis_index("blk")
    rows = q_ref.shape[0]
    wide = n * rows
    cached = kc_ref.shape[0]
    picked = path_hbm.shape[0]
    peers = [partner(me, k, n) for k in range(n - 1, 0, -1)]

    load_q = pltpu.make_async_copy(q_ref, qbuf.at[me], load_sem.at[0])
    load_q.start()
    small_loads = [
        pltpu.make_async_copy(src, dst, load_sem.at[4 + i])
        for i, (src, dst) in enumerate((
            (parents_hbm, parents_ref), (length_hbm, length_ref), (path_hbm, path_ref),
            (k_ref, kown), (v_ref, vown),
        ))
    ]
    for copy in small_loads:
        copy.start()
    load_k = pltpu.make_async_copy(kc_ref, kbuf, load_sem.at[1])
    load_v = pltpu.make_async_copy(vc_ref, vbuf, load_sem.at[2])
    load_w = pltpu.make_async_copy(w_ref, wbuf, load_sem.at[3])
    load_k.start()
    load_v.start()

    barrier = pltpu.get_barrier_semaphore()
    for peer in peers:
        pl.semaphore_signal(barrier, inc=1, device_id={"blk": peer}, device_id_type=MESH)
    pl.semaphore_wait(barrier, n - 1)

    def q_copy(c, peer):
        columns = pl.ds(c * CHUNK, CHUNK)
        return pltpu.make_async_remote_copy(
            src_ref=qbuf.at[me, :, columns], dst_ref=qbuf.at[me, :, columns],
            send_sem=sends.at[0], recv_sem=q_recv.at[c],
            device_id={"blk": peer}, device_id_type=MESH,
        )

    def r_copy(c, peer):
        return pltpu.make_async_remote_copy(
            src_ref=sbuf.at[c, peer], dst_ref=rbuf.at[c, me],
            send_sem=sends.at[1], recv_sem=r_recv.at[c],
            device_id={"blk": peer}, device_id_type=MESH,
        )

    def p_copy(c, peer):
        return pltpu.make_async_remote_copy(
            src_ref=psend.at[c], dst_ref=pbuf.at[c, me],
            send_sem=sends.at[2], recv_sem=p_recv.at[c],
            device_id={"blk": peer}, device_id_type=MESH,
        )

    def arrived(block, sem):
        pltpu.make_async_copy(block, block, sem).wait()

    others = pl.ds(0, n - 1)
    load_q.wait()
    for c in range(CHUNKS):
        for peer in peers:
            q_copy(c, peer).start()
    load_w.start()

    for copy in small_loads:
        copy.wait()

    up = lax.broadcasted_iota(jnp.int32, (wide, wide), 0)
    down = lax.broadcasted_iota(jnp.int32, (wide, wide), 1)
    up_node = up // rows * own + up % rows
    links = jnp.where(up == down, 1.0, 0.0)
    for i in range(1, nodes):
        at = i // own * rows + i % own
        links = jnp.where((down == at) & (up_node == parents_ref[i]) & (up % rows < own), 1.0, links)
    for squaring in range(max(1, math.ceil(math.log2(nodes)))):
        half = links.astype(jnp.bfloat16)
        links = jnp.minimum(jnp.dot(half, half, preferred_element_type=jnp.float32), 1.0)
    source = lax.broadcasted_iota(jnp.int32, (wide, LANES), 0)
    lane = lax.broadcasted_iota(jnp.int32, (wide, LANES), 1)
    spare = lane % HALF
    mine = jnp.where((source == me * rows + spare - 1) & (spare >= 1) & (spare <= own), 1.0, 0.0)
    related = lax.dot_general(
        links.astype(jnp.bfloat16), mine.astype(jnp.bfloat16), (((0,), (0,)), ((), ())),
        preferred_element_type=jnp.float32,
    )
    marks = jnp.where(
        spare == 0, 1.0,
        jnp.where((spare <= own) & (related < 0.5), EXCLUDED, 0.0),
    )

    size = n * HALF
    at = lax.broadcasted_iota(jnp.int32, (2 * size, LANES), 0)
    goal = lax.broadcasted_iota(jnp.int32, (2 * size, LANES), 1)
    spot_node = at % size // HALF * own + at % ROWS
    wanted = jnp.full((2 * size, LANES), -1, jnp.int32)
    for k in range(picked):
        wanted = jnp.where(goal % ROWS == k, path_ref[k], wanted)
    same = (at // size == goal // HALF) & (at % HALF // ROWS == goal % HALF // ROWS)
    picks[...] = jnp.where(
        same & (wanted == spot_node) & (at % ROWS < own), 1.0, 0.0
    ).astype(jnp.bfloat16)

    place = lax.broadcasted_iota(jnp.int32, (cached, LANES), 0) + me * cached
    column = lax.broadcasted_iota(jnp.int32, (cached, LANES), 1)
    spent = jnp.where((column % HALF == 0) & (place >= length_ref[0]), EXCLUDED, 0.0)
    node = lax.broadcasted_iota(jnp.int32, (TILE, LANES), 0)
    node_lane = lax.broadcasted_iota(jnp.int32, (TILE, LANES), 1)
    node_spare = node_lane % HALF
    tags = jnp.where(
        node < own, jnp.where(node_spare == node + 1, 1.0, 0.0),
        jnp.where(node_spare == 0, EXCLUDED, 0.0),
    )
    blank = jnp.zeros((LANES - rows, LANES), jnp.float32)
    load_k.wait()
    for h in range(KEY_VALUE_HEADS):
        columns = slice(h // 2 * LANES, (h // 2 + 1) * LANES)
        held = (column < HALF) if h % 2 == 0 else (column >= HALF)
        node_held = (node_lane < HALF) if h % 2 == 0 else (node_lane >= HALF)
        keys[h, pl.ds(0, cached)] = jnp.where(
            held, kbuf[:, columns].astype(jnp.float32), spent
        ).astype(jnp.bfloat16)
        fresh = jnp.concatenate([kown[:, columns].astype(jnp.float32), blank], axis=0)
        keys[h, pl.ds(cached, TILE)] = jnp.where(node_held, fresh[:TILE], tags).astype(jnp.bfloat16)
    load_v.wait()
    for c in range(CHUNKS):
        columns = slice(c * LANES, (c + 1) * LANES)
        fresh = jnp.concatenate([vown[:, columns].astype(jnp.float32), blank], axis=0)
        turned = vbuf[:, columns].astype(jnp.float32).T.astype(jnp.bfloat16)
        fresh = fresh.T.astype(jnp.bfloat16)
        for side in range(2):
            half = slice(side * HALF, (side + 1) * HALF)
            values[2 * c + side, pl.ds(0, HALF), pl.ds(0, cached)] = turned[half]
            values[2 * c + side, pl.ds(0, HALF), pl.ds(cached, LANES)] = fresh[half]
            values[2 * c + side, pl.ds(HALF, 16)] = jnp.ones((16, cached + LANES), jnp.bfloat16)

    low = lax.broadcasted_iota(jnp.int32, (rows, LANES), 1) < HALF
    deep_low = lax.broadcasted_iota(jnp.int32, (DEPTH, LANES), 1) < HALF
    for c in range(CHUNKS):
        arrived(qbuf.at[others, :, pl.ds(c * CHUNK, CHUNK)], q_recv.at[c])
        q = qbuf[:, :, c * CHUNK : (c + 1) * CHUNK].astype(jnp.float32)
        asked = []
        for side in range(2):
            keep = low if side == 0 else jnp.logical_not(low)
            stacked = []
            for d in range(n):
                extra = marks[d * rows : (d + 1) * rows]
                for pair in range(PAIRS):
                    start = side * SPAN + pair * LANES
                    tile = q[d, :, start : start + LANES]
                    turned = pltpu.roll(tile, HALF, 1)
                    even, odd = (tile, turned) if side == 0 else (turned, tile)
                    stacked.append(jnp.where(keep, even, extra))
                    stacked.append(jnp.where(keep, odd, extra))
            queries = jnp.concatenate(stacked, axis=0).astype(jnp.bfloat16)
            asked += [
                (2 * c + side, queries[start : start + UNIT]) for start in range(0, size, UNIT)
            ]

        def score(h, queries):
            return lax.dot_general(keys[h], queries, NT, preferred_element_type=jnp.float32)

        def weigh(h, scores):
            top = jnp.maximum(jnp.max(scores, axis=0, keepdims=True), FLOOR)
            weights = jnp.exp2((scores - top) * EXPONENT).astype(jnp.bfloat16)
            weighted = jnp.dot(
                values[h, :, pl.ds(0, cached)], weights[:cached], preferred_element_type=jnp.float32
            ) + jnp.dot(
                values[h, :, pl.ds(cached, TILE)], weights[cached:],
                preferred_element_type=jnp.float32,
            )
            return jnp.concatenate([weighted[:HALF], fold(top, weighted[HALF:DEPTH])], axis=0)

        done, waiting = [], []
        for h, queries in asked:
            waiting.append((h, score(h, queries)))
            if len(waiting) > LAG:
                done.append(weigh(*waiting.pop(0)))
        done += [weigh(*each) for each in waiting]
        per = len(done) // 2
        full = [jnp.concatenate(done[side * per : (side + 1) * per], axis=1) for side in range(2)]
        psend[c] = jnp.dot(
            jnp.concatenate(full, axis=1).astype(jnp.bfloat16), picks[...],
            preferred_element_type=jnp.float32,
        ).astype(jnp.bfloat16)
        for peer in peers:
            p_copy(c, peer).start()
        for d in range(n):
            block = slice(d // 2 * LANES, (d // 2 + 1) * LANES)
            left, right = full[0][:, block], full[1][:, block]
            if d % 2 == 0:
                right = pltpu.roll(right, HALF, 1)
            else:
                left = pltpu.roll(left, HALF, 1)
            sbuf[c, d] = jnp.where(deep_low, left, right).astype(jnp.bfloat16)
        for peer in peers:
            r_copy(c, peer).start()

    load_w.wait()
    acc[...] = jnp.zeros_like(acc)
    for c in range(CHUNKS):
        columns = pl.ds(c * CHUNK, CHUNK)
        arrived(pbuf.at[c, others], p_recv.at[c])
        parts = [psend[c]] + [pbuf[c, peer] for peer in peers]
        acc[...] += lax.dot_general(
            merge([part.astype(jnp.float32) for part in parts]), wbuf[:, columns], NT,
            preferred_element_type=jnp.float32,
        )
        if c == CHUNKS - 1:
            out_ref[...] = acc[...].astype(jnp.bfloat16)
        arrived(rbuf.at[c, others], r_recv.at[c])
        parts = [sbuf[c, me]] + [rbuf[c, peer] for peer in peers]
        att_ref[:, columns] = merge([part.astype(jnp.float32) for part in parts])

    arrived(qbuf.at[others], sends.at[0])
    arrived(rbuf.at[:, others], sends.at[1])
    arrived(pbuf.at[:, others], sends.at[2])


def write_out(att_ref, out_ref, att_hbm, out_hbm, sems):
    copies = [
        pltpu.make_async_copy(att_ref, att_hbm, sems.at[0]),
        pltpu.make_async_copy(out_ref, out_hbm, sems.at[1]),
    ]
    for copy in copies:
        copy.start()
    for copy in copies:
        copy.wait()


def local(
    n,
    draft_node_queries,
    draft_node_keys,
    draft_node_values,
    paged_key_cache,
    paged_value_cache,
    context_length,
    parents,
    accepted_path,
    out_weight,
):
    own = draft_node_queries.shape[0]
    rows = -(-own // 8) * 8
    if rows != own:
        pad = ((0, rows - own), (0, 0))
        draft_node_queries = jnp.pad(draft_node_queries, pad)
        draft_node_keys = jnp.pad(draft_node_keys, pad)
        draft_node_values = jnp.pad(draft_node_values, pad)
    cached, cache_width = paged_key_cache.shape
    picked = accepted_path.shape[0]
    q_width = QUERY_HEADS * HEAD_WIDTH
    vmem = pl.BlockSpec(memory_space=pltpu.VMEM)
    anywhere = pl.BlockSpec(memory_space=pltpu.HBM)
    shapes = (
        jax.ShapeDtypeStruct((rows, q_width), jnp.bfloat16),
        jax.ShapeDtypeStruct((picked, out_weight.shape[0]), jnp.bfloat16),
    )
    held = pl.pallas_call(
        functools.partial(kernel, n, own, parents.shape[0]),
        out_shape=tuple(pltpu.VMEM(shape.shape, shape.dtype) for shape in shapes),
        in_specs=[anywhere] * 9,
        out_specs=(vmem, vmem),
        scratch_shapes=[
            pltpu.SMEM(context_length.shape, jnp.int32),
            pltpu.SMEM(parents.shape, jnp.int32),
            pltpu.SMEM(accepted_path.shape, jnp.int32),
            pltpu.VMEM((rows, cache_width), jnp.bfloat16),
            pltpu.VMEM((rows, cache_width), jnp.bfloat16),
            pltpu.VMEM((n, rows, q_width), jnp.bfloat16),
            pltpu.VMEM((cached, cache_width), jnp.bfloat16),
            pltpu.VMEM((cached, cache_width), jnp.bfloat16),
            pltpu.VMEM(out_weight.shape, jnp.bfloat16),
            pltpu.VMEM((KEY_VALUE_HEADS, cached + TILE, LANES), jnp.bfloat16),
            pltpu.VMEM((KEY_VALUE_HEADS, HALF + 16, cached + LANES), jnp.bfloat16),
            pltpu.VMEM((CHUNKS, n, DEPTH, LANES), jnp.bfloat16),
            pltpu.VMEM((CHUNKS, n, DEPTH, LANES), jnp.bfloat16),
            pltpu.VMEM((CHUNKS, DEPTH, LANES), jnp.bfloat16),
            pltpu.VMEM((CHUNKS, n, DEPTH, LANES), jnp.bfloat16),
            pltpu.VMEM((2 * n * HALF, LANES), jnp.bfloat16),
            pltpu.VMEM((picked, out_weight.shape[0]), jnp.float32),
            pltpu.SemaphoreType.DMA((9,)),
            pltpu.SemaphoreType.DMA((CHUNKS,)),
            pltpu.SemaphoreType.DMA((CHUNKS,)),
            pltpu.SemaphoreType.DMA((CHUNKS,)),
            pltpu.SemaphoreType.DMA((3,)),
        ],
        compiler_params=pltpu.CompilerParams(
            collective_id=0, has_side_effects=True, vmem_limit_bytes=56 * 1024 * 1024
        ),
        name="verify_tree",
    )(
        context_length, parents, accepted_path,
        draft_node_queries, draft_node_keys, draft_node_values,
        paged_key_cache, paged_value_cache, out_weight,
    )
    attention, path_output = pl.pallas_call(
        write_out,
        out_shape=shapes,
        in_specs=(vmem, vmem),
        out_specs=(anywhere, anywhere),
        scratch_shapes=[pltpu.SemaphoreType.DMA((2,))],
        compiler_params=pltpu.CompilerParams(vmem_limit_bytes=1024 * 1024),
        name="write_out",
    )(*held)
    return attention[:own], path_output


def solution(mesh):
    in_specs = (
        P(("req", "blk"), None),
        P(("req", "blk"), None),
        P(("req", "blk"), None),
        P(("req", "blk"), None),
        P(("req", "blk"), None),
        P("req"),
        P("req"),
        P("req"),
        P("blk", None),
    )
    out_specs = (P(("req", "blk"), None), P("req", "blk"))
    return jax.shard_map(
        functools.partial(local, mesh.shape["blk"]),
        mesh=mesh, in_specs=in_specs, out_specs=out_specs, check_vma=False,
    )
```

```python
import functools
import math

import jax
import jax.numpy as jnp
from jax import lax
from jax.experimental import pallas as pl
from jax.experimental.pallas import tpu as pltpu
from jax.sharding import PartitionSpec as P

QUERY_HEADS = 64
KEY_VALUE_HEADS = 8
HEAD_WIDTH = 64
GROUP = QUERY_HEADS // KEY_VALUE_HEADS
LANES = 128
HALF = LANES // 2
SPAN = GROUP * HEAD_WIDTH
PAIRS = SPAN // LANES
CHUNKS = KEY_VALUE_HEADS // 2
CHUNK = 2 * SPAN
ROWS = LANES // (2 * GROUP)
DEPTH = HEAD_WIDTH + 8
TILE = 16
EXCLUDED = -1e30
FLOOR = -1e20
SCALE = HEAD_WIDTH ** (-0.5)
EXPONENT = SCALE * math.log2(math.e)
NT = (((1,), (1,)), ((), ()))
MESH = pl.DeviceIdType.MESH


def partner(me, k, n):
    if n & (n - 1):
        return lax.rem(me + k, n)
    other = me
    bit = 1
    while bit < n:
        if k & bit:
            other = other + bit - 2 * bit * ((me // bit) % 2)
        bit *= 2
    return other


def split(value):
    first = value.astype(jnp.bfloat16).astype(jnp.float32)
    rest = value - first
    second = rest.astype(jnp.bfloat16).astype(jnp.float32)
    return [first, second, rest - second]


def fold(top, total):
    row = lax.broadcasted_iota(jnp.int32, total.shape, 0)
    stat = jnp.zeros_like(total)
    for at, term in enumerate(split(jnp.broadcast_to(top, total.shape)) + split(total)):
        stat = jnp.where(row == at, term, stat)
    return stat


def merge(parts):
    stats = [part[HEAD_WIDTH:] for part in parts]
    tops = [stat[0:1] + stat[1:2] + stat[2:3] for stat in stats]
    totals = [stat[3:4] + stat[4:5] + stat[5:6] for stat in stats]
    top = functools.reduce(jnp.maximum, tops)
    shares = [jnp.exp2((each - top) * EXPONENT) for each in tops]
    total = functools.reduce(jnp.add, [share * each for share, each in zip(shares, totals)])
    merged = functools.reduce(
        jnp.add, [part[:HEAD_WIDTH] * (share / total) for share, part in zip(shares, parts)]
    )
    turned = jnp.concatenate([merged, pltpu.roll(merged, LANES - ROWS, 1)], axis=0).T
    return jnp.concatenate(
        [turned[2 * ROWS * pair : 2 * ROWS * pair + ROWS] for pair in range(2 * PAIRS)], axis=1
    ).astype(jnp.bfloat16)


def kernel(
    n, own, nodes,
    length_hbm, parents_hbm, path_hbm, q_ref, k_ref, v_ref, kc_ref, vc_ref, w_ref,
    att_ref, out_ref,
    length_ref, parents_ref, path_ref, kown, vown,
    qbuf, kbuf, vbuf, wbuf, keys, values, sbuf, rbuf, psend, pbuf, picks, acc,
    load_sem, q_recv, r_recv, p_recv, sends,
):
    me = lax.axis_index("blk")
    rows = q_ref.shape[0]
    wide = n * rows
    cached = kc_ref.shape[0]
    picked = path_hbm.shape[0]
    peers = [partner(me, k, n) for k in range(n - 1, 0, -1)]

    load_q = pltpu.make_async_copy(q_ref, qbuf.at[me], load_sem.at[0])
    load_q.start()
    barrier = pltpu.get_barrier_semaphore()
    for peer in peers:
        pl.semaphore_signal(barrier, inc=1, device_id={"blk": peer}, device_id_type=MESH)
    small_loads = [
        pltpu.make_async_copy(src, dst, load_sem.at[4 + i])
        for i, (src, dst) in enumerate((
            (parents_hbm, parents_ref), (length_hbm, length_ref), (path_hbm, path_ref),
            (k_ref, kown), (v_ref, vown),
        ))
    ]
    for copy in small_loads:
        copy.start()
    load_k = pltpu.make_async_copy(kc_ref, kbuf, load_sem.at[1])
    load_v = pltpu.make_async_copy(vc_ref, vbuf, load_sem.at[2])
    load_w = pltpu.make_async_copy(w_ref, wbuf, load_sem.at[3])
    load_k.start()
    load_v.start()

    pl.semaphore_wait(barrier, n - 1)

    def q_copy(c, peer):
        columns = pl.ds(c * CHUNK, CHUNK)
        return pltpu.make_async_remote_copy(
            src_ref=qbuf.at[me, :, columns], dst_ref=qbuf.at[me, :, columns],
            send_sem=sends.at[0], recv_sem=q_recv.at[c],
            device_id={"blk": peer}, device_id_type=MESH,
        )

    def r_copy(c, peer):
        return pltpu.make_async_remote_copy(
            src_ref=sbuf.at[c, peer], dst_ref=rbuf.at[c, me],
            send_sem=sends.at[1], recv_sem=r_recv.at[c],
            device_id={"blk": peer}, device_id_type=MESH,
        )

    def p_copy(c, peer):
        return pltpu.make_async_remote_copy(
            src_ref=psend.at[c], dst_ref=pbuf.at[c, me],
            send_sem=sends.at[2], recv_sem=p_recv.at[c],
            device_id={"blk": peer}, device_id_type=MESH,
        )

    def arrived(block, sem):
        pltpu.make_async_copy(block, block, sem).wait()

    others = pl.ds(0, n - 1)
    load_q.wait()
    for c in range(CHUNKS):
        for peer in peers:
            q_copy(c, peer).start()
    load_w.start()

    for copy in small_loads:
        copy.wait()

    up = lax.broadcasted_iota(jnp.int32, (wide, wide), 0)
    down = lax.broadcasted_iota(jnp.int32, (wide, wide), 1)
    up_node = up // rows * own + up % rows
    links = jnp.where(up == down, 1.0, 0.0)
    for i in range(1, nodes):
        at = i // own * rows + i % own
        links = jnp.where((down == at) & (up_node == parents_ref[i]) & (up % rows < own), 1.0, links)
    for squaring in range(max(1, math.ceil(math.log2(nodes)))):
        half = links.astype(jnp.bfloat16)
        links = jnp.minimum(jnp.dot(half, half, preferred_element_type=jnp.float32), 1.0)
    source = lax.broadcasted_iota(jnp.int32, (wide, LANES), 0)
    lane = lax.broadcasted_iota(jnp.int32, (wide, LANES), 1)
    spare = lane % HALF
    mine = jnp.where((source == me * rows + spare - 1) & (spare >= 1) & (spare <= own), 1.0, 0.0)
    related = lax.dot_general(
        links.astype(jnp.bfloat16), mine.astype(jnp.bfloat16), (((0,), (0,)), ((), ())),
        preferred_element_type=jnp.float32,
    )
    marks = jnp.where(
        spare == 0, 1.0,
        jnp.where((spare <= own) & (related < 0.5), EXCLUDED, 0.0),
    )

    size = n * HALF
    at = lax.broadcasted_iota(jnp.int32, (2 * size, LANES), 0)
    goal = lax.broadcasted_iota(jnp.int32, (2 * size, LANES), 1)
    spot_node = at % size // HALF * own + at % ROWS
    wanted = jnp.full((2 * size, LANES), -1, jnp.int32)
    for k in range(picked):
        wanted = jnp.where(goal % ROWS == k, path_ref[k], wanted)
    same = (at // size == goal // HALF) & (at % HALF // ROWS == goal % HALF // ROWS)
    picks[...] = jnp.where(
        same & (wanted == spot_node) & (at % ROWS < own), 1.0, 0.0
    ).astype(jnp.bfloat16)

    place = lax.broadcasted_iota(jnp.int32, (cached, LANES), 0) + me * cached
    column = lax.broadcasted_iota(jnp.int32, (cached, LANES), 1)
    spent = jnp.where((column % HALF == 0) & (place >= length_ref[0]), EXCLUDED, 0.0)
    node = lax.broadcasted_iota(jnp.int32, (TILE, LANES), 0)
    node_lane = lax.broadcasted_iota(jnp.int32, (TILE, LANES), 1)
    node_spare = node_lane % HALF
    tags = jnp.where(
        node < own, jnp.where(node_spare == node + 1, 1.0, 0.0),
        jnp.where(node_spare == 0, EXCLUDED, 0.0),
    )
    blank = jnp.zeros((LANES - rows, LANES), jnp.float32)
    load_k.wait()
    for h in range(KEY_VALUE_HEADS):
        columns = slice(h // 2 * LANES, (h // 2 + 1) * LANES)
        held = (column < HALF) if h % 2 == 0 else (column >= HALF)
        node_held = (node_lane < HALF) if h % 2 == 0 else (node_lane >= HALF)
        keys[h, pl.ds(0, cached)] = jnp.where(
            held, kbuf[:, columns].astype(jnp.float32), spent
        ).astype(jnp.bfloat16)
        fresh = jnp.concatenate([kown[:, columns].astype(jnp.float32), blank], axis=0)
        keys[h, pl.ds(cached, TILE)] = jnp.where(node_held, fresh[:TILE], tags).astype(jnp.bfloat16)
    load_v.wait()
    for c in range(CHUNKS):
        columns = slice(c * LANES, (c + 1) * LANES)
        fresh = jnp.concatenate([vown[:, columns].astype(jnp.float32), blank], axis=0)
        turned = vbuf[:, columns].astype(jnp.float32).T.astype(jnp.bfloat16)
        fresh = fresh.T.astype(jnp.bfloat16)
        for side in range(2):
            half = slice(side * HALF, (side + 1) * HALF)
            values[2 * c + side, pl.ds(0, HALF), pl.ds(0, cached)] = turned[half]
            values[2 * c + side, pl.ds(0, HALF), pl.ds(cached, LANES)] = fresh[half]
            values[2 * c + side, pl.ds(HALF, 16)] = jnp.ones((16, cached + LANES), jnp.bfloat16)

    low = lax.broadcasted_iota(jnp.int32, (rows, LANES), 1) < HALF
    deep_low = lax.broadcasted_iota(jnp.int32, (DEPTH, LANES), 1) < HALF
    def ask(h):
        side = h % 2
        columns = pl.ds(h * SPAN, SPAN)
        q = qbuf[:, :, columns].astype(jnp.float32)
        keep = low if side == 0 else jnp.logical_not(low)
        stacked = []
        for d in range(n):
            extra = marks[d * rows : (d + 1) * rows]
            for pair in range(PAIRS):
                start = pair * LANES
                tile = q[d, :, start : start + LANES]
                turned = pltpu.roll(tile, HALF, 1)
                even, odd = (tile, turned) if side == 0 else (turned, tile)
                stacked.append(jnp.where(keep, even, extra))
                stacked.append(jnp.where(keep, odd, extra))
        queries = jnp.concatenate(stacked, axis=0).astype(jnp.bfloat16)
        return lax.dot_general(keys[h], queries, NT, preferred_element_type=jnp.float32)

    def weigh(h, scores):
        top = jnp.maximum(jnp.max(scores, axis=0, keepdims=True), FLOOR)
        weights = jnp.exp2((scores - top) * EXPONENT).astype(jnp.bfloat16)
        weighted = jnp.dot(
            values[h, :, pl.ds(0, cached)], weights[:cached], preferred_element_type=jnp.float32
        ) + jnp.dot(
            values[h, :, pl.ds(cached, TILE)], weights[cached:],
            preferred_element_type=jnp.float32,
        )
        return jnp.concatenate([weighted[:HALF], fold(top, weighted[HALF:DEPTH])], axis=0)

    def reach(c):
        arrived(qbuf.at[others, :, pl.ds(c * CHUNK, CHUNK)], q_recv.at[c])

    ahead = []
    for c in range(CHUNKS):
        if not ahead:
            reach(c)
            ahead = [ask(2 * c), ask(2 * c + 1)]
        full, scores, ahead = [], ahead, []
        early = 0 <= c < CHUNKS - 1
        if early:
            reach(c + 1)
        for side in range(2):
            if early:
                ahead.append(ask(2 * c + 2 + side))
            full.append(weigh(2 * c + side, scores[side]))
        psend[c] = jnp.dot(
            jnp.concatenate(full, axis=1).astype(jnp.bfloat16), picks[...],
            preferred_element_type=jnp.float32,
        ).astype(jnp.bfloat16)
        for peer in peers:
            p_copy(c, peer).start()
        for d in range(n):
            block = slice(d // 2 * LANES, (d // 2 + 1) * LANES)
            left, right = full[0][:, block], full[1][:, block]
            if d % 2 == 0:
                right = pltpu.roll(right, HALF, 1)
            else:
                left = pltpu.roll(left, HALF, 1)
            sbuf[c, d] = jnp.where(deep_low, left, right).astype(jnp.bfloat16)
        for peer in peers:
            r_copy(c, peer).start()

    load_w.wait()
    acc[...] = jnp.zeros_like(acc)
    for c in range(CHUNKS):
        columns = pl.ds(c * CHUNK, CHUNK)
        arrived(pbuf.at[c, others], p_recv.at[c])
        parts = [psend[c]] + [pbuf[c, peer] for peer in peers]
        acc[...] += lax.dot_general(
            merge([part.astype(jnp.float32) for part in parts]), wbuf[:, columns], NT,
            preferred_element_type=jnp.float32,
        )
        if c == CHUNKS - 1:
            out_ref[...] = acc[...].astype(jnp.bfloat16)
        arrived(rbuf.at[c, others], r_recv.at[c])
        parts = [sbuf[c, me]] + [rbuf[c, peer] for peer in peers]
        att_ref[:, columns] = merge([part.astype(jnp.float32) for part in parts])

    arrived(qbuf.at[others], sends.at[0])
    arrived(rbuf.at[:, others], sends.at[1])
    arrived(pbuf.at[:, others], sends.at[2])


def write_out(att_ref, out_ref, att_hbm, out_hbm, sems):
    copies = [
        pltpu.make_async_copy(att_ref, att_hbm, sems.at[0]),
        pltpu.make_async_copy(out_ref, out_hbm, sems.at[1]),
    ]
    for copy in copies:
        copy.start()
    for copy in copies:
        copy.wait()


def local(
    n,
    draft_node_queries,
    draft_node_keys,
    draft_node_values,
    paged_key_cache,
    paged_value_cache,
    context_length,
    parents,
    accepted_path,
    out_weight,
):
    own = draft_node_queries.shape[0]
    rows = -(-own // 8) * 8
    if rows != own:
        pad = ((0, rows - own), (0, 0))
        draft_node_queries = jnp.pad(draft_node_queries, pad)
        draft_node_keys = jnp.pad(draft_node_keys, pad)
        draft_node_values = jnp.pad(draft_node_values, pad)
    cached, cache_width = paged_key_cache.shape
    picked = accepted_path.shape[0]
    q_width = QUERY_HEADS * HEAD_WIDTH
    vmem = pl.BlockSpec(memory_space=pltpu.VMEM)
    anywhere = pl.BlockSpec(memory_space=pltpu.HBM)
    shapes = (
        jax.ShapeDtypeStruct((rows, q_width), jnp.bfloat16),
        jax.ShapeDtypeStruct((picked, out_weight.shape[0]), jnp.bfloat16),
    )
    held = pl.pallas_call(
        functools.partial(kernel, n, own, parents.shape[0]),
        out_shape=tuple(pltpu.VMEM(shape.shape, shape.dtype) for shape in shapes),
        in_specs=[anywhere] * 9,
        out_specs=(vmem, vmem),
        scratch_shapes=[
            pltpu.SMEM(context_length.shape, jnp.int32),
            pltpu.SMEM(parents.shape, jnp.int32),
            pltpu.SMEM(accepted_path.shape, jnp.int32),
            pltpu.VMEM((rows, cache_width), jnp.bfloat16),
            pltpu.VMEM((rows, cache_width), jnp.bfloat16),
            pltpu.VMEM((n, rows, q_width), jnp.bfloat16),
            pltpu.VMEM((cached, cache_width), jnp.bfloat16),
            pltpu.VMEM((cached, cache_width), jnp.bfloat16),
            pltpu.VMEM(out_weight.shape, jnp.bfloat16),
            pltpu.VMEM((KEY_VALUE_HEADS, cached + TILE, LANES), jnp.bfloat16),
            pltpu.VMEM((KEY_VALUE_HEADS, HALF + 16, cached + LANES), jnp.bfloat16),
            pltpu.VMEM((CHUNKS, n, DEPTH, LANES), jnp.bfloat16),
            pltpu.VMEM((CHUNKS, n, DEPTH, LANES), jnp.bfloat16),
            pltpu.VMEM((CHUNKS, DEPTH, LANES), jnp.bfloat16),
            pltpu.VMEM((CHUNKS, n, DEPTH, LANES), jnp.bfloat16),
            pltpu.VMEM((2 * n * HALF, LANES), jnp.bfloat16),
            pltpu.VMEM((picked, out_weight.shape[0]), jnp.float32),
            pltpu.SemaphoreType.DMA((9,)),
            pltpu.SemaphoreType.DMA((CHUNKS,)),
            pltpu.SemaphoreType.DMA((CHUNKS,)),
            pltpu.SemaphoreType.DMA((CHUNKS,)),
            pltpu.SemaphoreType.DMA((3,)),
        ],
        compiler_params=pltpu.CompilerParams(
            collective_id=0, has_side_effects=True, vmem_limit_bytes=56 * 1024 * 1024
        ),
        name="verify_tree",
    )(
        context_length, parents, accepted_path,
        draft_node_queries, draft_node_keys, draft_node_values,
        paged_key_cache, paged_value_cache, out_weight,
    )
    attention, path_output = pl.pallas_call(
        write_out,
        out_shape=shapes,
        in_specs=(vmem, vmem),
        out_specs=(anywhere, anywhere),
        scratch_shapes=[pltpu.SemaphoreType.DMA((2,))],
        compiler_params=pltpu.CompilerParams(vmem_limit_bytes=1024 * 1024),
        name="write_out",
    )(*held)
    return attention[:own], path_output


def solution(mesh):
    in_specs = (
        P(("req", "blk"), None),
        P(("req", "blk"), None),
        P(("req", "blk"), None),
        P(("req", "blk"), None),
        P(("req", "blk"), None),
        P("req"),
        P("req"),
        P("req"),
        P("blk", None),
    )
    out_specs = (P(("req", "blk"), None), P("req", "blk"))
    return jax.shard_map(
        functools.partial(local, mesh.shape["blk"]),
        mesh=mesh, in_specs=in_specs, out_specs=out_specs, check_vma=False,
    )
```

```python
import functools
import math

import jax
import jax.numpy as jnp
from jax import lax
from jax.experimental import pallas as pl
from jax.experimental.pallas import tpu as pltpu
from jax.sharding import PartitionSpec as P

QUERY_HEADS = 64
KEY_VALUE_HEADS = 8
HEAD_WIDTH = 64
GROUP = QUERY_HEADS // KEY_VALUE_HEADS
LANES = 128
HALF = LANES // 2
SPAN = GROUP * HEAD_WIDTH
PAIRS = SPAN // LANES
CHUNKS = KEY_VALUE_HEADS // 2
CHUNK = 2 * SPAN
ROWS = LANES // (2 * GROUP)
DEPTH = HEAD_WIDTH + 8
TILE = 16
EXCLUDED = -1e30
FLOOR = -1e20
SCALE = HEAD_WIDTH ** (-0.5)
EXPONENT = SCALE * math.log2(math.e)
NT = (((1,), (1,)), ((), ()))
MESH = pl.DeviceIdType.MESH


def partner(me, k, n):
    if n & (n - 1):
        return lax.rem(me + k, n)
    other = me
    bit = 1
    while bit < n:
        if k & bit:
            other = other + bit - 2 * bit * ((me // bit) % 2)
        bit *= 2
    return other


def split(value):
    first = value.astype(jnp.bfloat16).astype(jnp.float32)
    rest = value - first
    second = rest.astype(jnp.bfloat16).astype(jnp.float32)
    return [first, second, rest - second]


def fold(top, total):
    row = lax.broadcasted_iota(jnp.int32, total.shape, 0)
    stat = jnp.zeros_like(total)
    for at, term in enumerate(split(jnp.broadcast_to(top, total.shape)) + split(total)):
        stat = jnp.where(row == at, term, stat)
    return stat


def merge(parts):
    stats = [part[HEAD_WIDTH:] for part in parts]
    tops = [stat[0:1] + stat[1:2] + stat[2:3] for stat in stats]
    totals = [stat[3:4] + stat[4:5] + stat[5:6] for stat in stats]
    top = functools.reduce(jnp.maximum, tops)
    shares = [jnp.exp2((each - top) * EXPONENT) for each in tops]
    total = functools.reduce(jnp.add, [share * each for share, each in zip(shares, totals)])
    merged = functools.reduce(
        jnp.add, [part[:HEAD_WIDTH] * (share / total) for share, part in zip(shares, parts)]
    )
    turned = jnp.concatenate([merged, pltpu.roll(merged, LANES - ROWS, 1)], axis=0).T
    return jnp.concatenate(
        [turned[2 * ROWS * pair : 2 * ROWS * pair + ROWS] for pair in range(2 * PAIRS)], axis=1
    ).astype(jnp.bfloat16)


def kernel(
    n, own, nodes,
    length_hbm, parents_hbm, path_hbm, q_ref, k_ref, v_ref, kc_ref, vc_ref, w_ref,
    att_ref, out_ref,
    length_ref, parents_ref, path_ref, kown, vown,
    qbuf, kbuf, vbuf, wbuf, keys, values, sbuf, rbuf, psend, pbuf, picks, acc,
    load_sem, q_recv, r_recv, p_recv, sends,
):
    me = lax.axis_index("blk")
    rows = q_ref.shape[0]
    wide = n * rows
    cached = kc_ref.shape[0]
    picked = path_hbm.shape[0]
    peers = [partner(me, k, n) for k in range(n - 1, 0, -1)]

    load_q = pltpu.make_async_copy(q_ref, qbuf.at[me], load_sem.at[0])
    load_q.start()
    barrier = pltpu.get_barrier_semaphore()
    for peer in peers:
        pl.semaphore_signal(barrier, inc=1, device_id={"blk": peer}, device_id_type=MESH)
    small_loads = [
        pltpu.make_async_copy(src, dst, load_sem.at[4 + i])
        for i, (src, dst) in enumerate((
            (parents_hbm, parents_ref), (length_hbm, length_ref), (path_hbm, path_ref),
            (k_ref, kown), (v_ref, vown),
        ))
    ]
    for copy in small_loads:
        copy.start()
    load_k = pltpu.make_async_copy(kc_ref, kbuf, load_sem.at[1])
    load_v = pltpu.make_async_copy(vc_ref, vbuf, load_sem.at[2])
    load_w = pltpu.make_async_copy(w_ref, wbuf, load_sem.at[3])
    load_k.start()
    load_v.start()
    load_w.start()

    pl.semaphore_wait(barrier, n - 1)

    def q_copy(c, peer):
        columns = pl.ds(c * CHUNK, CHUNK)
        return pltpu.make_async_remote_copy(
            src_ref=qbuf.at[me, :, columns], dst_ref=qbuf.at[me, :, columns],
            send_sem=sends.at[0], recv_sem=q_recv.at[c],
            device_id={"blk": peer}, device_id_type=MESH,
        )

    def r_copy(c, peer):
        return pltpu.make_async_remote_copy(
            src_ref=sbuf.at[c, peer], dst_ref=rbuf.at[c, me],
            send_sem=sends.at[1], recv_sem=r_recv.at[c],
            device_id={"blk": peer}, device_id_type=MESH,
        )

    def p_copy(c, peer):
        return pltpu.make_async_remote_copy(
            src_ref=psend.at[c], dst_ref=pbuf.at[c, me],
            send_sem=sends.at[2], recv_sem=p_recv.at[c],
            device_id={"blk": peer}, device_id_type=MESH,
        )

    def arrived(block, sem):
        pltpu.make_async_copy(block, block, sem).wait()

    others = pl.ds(0, n - 1)
    load_q.wait()
    for c in range(CHUNKS):
        for peer in peers:
            q_copy(c, peer).start()

    for copy in small_loads:
        copy.wait()

    up = lax.broadcasted_iota(jnp.int32, (wide, wide), 0)
    down = lax.broadcasted_iota(jnp.int32, (wide, wide), 1)
    up_node = up // rows * own + up % rows
    links = jnp.where(up == down, 1.0, 0.0)
    for i in range(1, nodes):
        at = i // own * rows + i % own
        links = jnp.where((down == at) & (up_node == parents_ref[i]) & (up % rows < own), 1.0, links)
    for squaring in range(max(1, math.ceil(math.log2(nodes)))):
        half = links.astype(jnp.bfloat16)
        links = jnp.minimum(jnp.dot(half, half, preferred_element_type=jnp.float32), 1.0)
    source = lax.broadcasted_iota(jnp.int32, (wide, LANES), 0)
    lane = lax.broadcasted_iota(jnp.int32, (wide, LANES), 1)
    spare = lane % HALF
    mine = jnp.where((source == me * rows + spare - 1) & (spare >= 1) & (spare <= own), 1.0, 0.0)
    related = lax.dot_general(
        links.astype(jnp.bfloat16), mine.astype(jnp.bfloat16), (((0,), (0,)), ((), ())),
        preferred_element_type=jnp.float32,
    )
    marks = jnp.where(
        spare == 0, 1.0,
        jnp.where((spare <= own) & (related < 0.5), EXCLUDED, 0.0),
    )

    size = n * HALF
    at = lax.broadcasted_iota(jnp.int32, (2 * size, LANES), 0)
    goal = lax.broadcasted_iota(jnp.int32, (2 * size, LANES), 1)
    spot_node = at % size // HALF * own + at % ROWS
    wanted = jnp.full((2 * size, LANES), -1, jnp.int32)
    for k in range(picked):
        wanted = jnp.where(goal % ROWS == k, path_ref[k], wanted)
    same = (at // size == goal // HALF) & (at % HALF // ROWS == goal % HALF // ROWS)
    picks[...] = jnp.where(
        same & (wanted == spot_node) & (at % ROWS < own), 1.0, 0.0
    ).astype(jnp.bfloat16)

    place = lax.broadcasted_iota(jnp.int32, (cached, LANES), 0) + me * cached
    column = lax.broadcasted_iota(jnp.int32, (cached, LANES), 1)
    spent = jnp.where((column % HALF == 0) & (place >= length_ref[0]), EXCLUDED, 0.0)
    node = lax.broadcasted_iota(jnp.int32, (TILE, LANES), 0)
    node_lane = lax.broadcasted_iota(jnp.int32, (TILE, LANES), 1)
    node_spare = node_lane % HALF
    tags = jnp.where(
        node < own, jnp.where(node_spare == node + 1, 1.0, 0.0),
        jnp.where(node_spare == 0, EXCLUDED, 0.0),
    )
    blank = jnp.zeros((LANES - rows, LANES), jnp.float32)
    load_k.wait()
    for h in range(KEY_VALUE_HEADS):
        columns = slice(h // 2 * LANES, (h // 2 + 1) * LANES)
        held = (column < HALF) if h % 2 == 0 else (column >= HALF)
        node_held = (node_lane < HALF) if h % 2 == 0 else (node_lane >= HALF)
        keys[h, pl.ds(0, cached)] = jnp.where(
            held, kbuf[:, columns].astype(jnp.float32), spent
        ).astype(jnp.bfloat16)
        fresh = jnp.concatenate([kown[:, columns].astype(jnp.float32), blank], axis=0)
        keys[h, pl.ds(cached, TILE)] = jnp.where(node_held, fresh[:TILE], tags).astype(jnp.bfloat16)
    load_v.wait()
    for c in range(CHUNKS):
        columns = slice(c * LANES, (c + 1) * LANES)
        fresh = jnp.concatenate([vown[:, columns].astype(jnp.float32), blank], axis=0)
        turned = vbuf[:, columns].astype(jnp.float32).T.astype(jnp.bfloat16)
        fresh = fresh.T.astype(jnp.bfloat16)
        for side in range(2):
            half = slice(side * HALF, (side + 1) * HALF)
            values[2 * c + side, pl.ds(0, HALF), pl.ds(0, cached)] = turned[half]
            values[2 * c + side, pl.ds(0, HALF), pl.ds(cached, LANES)] = fresh[half]
            values[2 * c + side, pl.ds(HALF, 16)] = jnp.ones((16, cached + LANES), jnp.bfloat16)

    low = lax.broadcasted_iota(jnp.int32, (rows, LANES), 1) < HALF
    deep_low = lax.broadcasted_iota(jnp.int32, (DEPTH, LANES), 1) < HALF
    def ask(h):
        side = h % 2
        columns = pl.ds(h * SPAN, SPAN)
        q = qbuf[:, :, columns].astype(jnp.float32)
        keep = low if side == 0 else jnp.logical_not(low)
        stacked = []
        for d in range(n):
            extra = marks[d * rows : (d + 1) * rows]
            for pair in range(PAIRS):
                start = pair * LANES
                tile = q[d, :, start : start + LANES]
                turned = pltpu.roll(tile, HALF, 1)
                even, odd = (tile, turned) if side == 0 else (turned, tile)
                stacked.append(jnp.where(keep, even, extra))
                stacked.append(jnp.where(keep, odd, extra))
        queries = jnp.concatenate(stacked, axis=0).astype(jnp.bfloat16)
        return lax.dot_general(keys[h], queries, NT, preferred_element_type=jnp.float32)

    def weigh(h, scores):
        top = jnp.maximum(jnp.max(scores, axis=0, keepdims=True), FLOOR)
        weights = jnp.exp2((scores - top) * EXPONENT).astype(jnp.bfloat16)
        weighted = jnp.dot(
            values[h, :, pl.ds(0, cached)], weights[:cached], preferred_element_type=jnp.float32
        ) + jnp.dot(
            values[h, :, pl.ds(cached, TILE)], weights[cached:],
            preferred_element_type=jnp.float32,
        )
        return jnp.concatenate([weighted[:HALF], fold(top, weighted[HALF:DEPTH])], axis=0)

    def reach(c):
        arrived(qbuf.at[others, :, pl.ds(c * CHUNK, CHUNK)], q_recv.at[c])

    ahead = []
    for c in range(CHUNKS):
        if not ahead:
            reach(c)
            ahead = [ask(2 * c), ask(2 * c + 1)]
        full, scores, ahead = [], ahead, []
        early = 0 <= c < CHUNKS - 1
        if early:
            reach(c + 1)
        for side in range(2):
            if early:
                ahead.append(ask(2 * c + 2 + side))
            full.append(weigh(2 * c + side, scores[side]))
        psend[c] = jnp.dot(
            jnp.concatenate(full, axis=1).astype(jnp.bfloat16), picks[...],
            preferred_element_type=jnp.float32,
        ).astype(jnp.bfloat16)
        for peer in peers:
            p_copy(c, peer).start()
        for d in range(n):
            block = slice(d // 2 * LANES, (d // 2 + 1) * LANES)
            left, right = full[0][:, block], full[1][:, block]
            if d % 2 == 0:
                right = pltpu.roll(right, HALF, 1)
            else:
                left = pltpu.roll(left, HALF, 1)
            sbuf[c, d] = jnp.where(deep_low, left, right).astype(jnp.bfloat16)
        for peer in peers:
            r_copy(c, peer).start()

    load_w.wait()
    acc[...] = jnp.zeros_like(acc)
    for c in range(CHUNKS):
        columns = pl.ds(c * CHUNK, CHUNK)
        arrived(pbuf.at[c, others], p_recv.at[c])
        parts = [psend[c]] + [pbuf[c, peer] for peer in peers]
        acc[...] += lax.dot_general(
            merge([part.astype(jnp.float32) for part in parts]), wbuf[:, columns], NT,
            preferred_element_type=jnp.float32,
        )
        if c == CHUNKS - 1:
            out_ref[...] = acc[...].astype(jnp.bfloat16)
        arrived(rbuf.at[c, others], r_recv.at[c])
        parts = [sbuf[c, me]] + [rbuf[c, peer] for peer in peers]
        att_ref[:, columns] = merge([part.astype(jnp.float32) for part in parts])

    arrived(qbuf.at[others], sends.at[0])
    arrived(rbuf.at[:, others], sends.at[1])
    arrived(pbuf.at[:, others], sends.at[2])


def write_out(att_ref, out_ref, att_hbm, out_hbm, sems):
    copies = [
        pltpu.make_async_copy(att_ref, att_hbm, sems.at[0]),
        pltpu.make_async_copy(out_ref, out_hbm, sems.at[1]),
    ]
    for copy in copies:
        copy.start()
    for copy in copies:
        copy.wait()


def local(
    n,
    draft_node_queries,
    draft_node_keys,
    draft_node_values,
    paged_key_cache,
    paged_value_cache,
    context_length,
    parents,
    accepted_path,
    out_weight,
):
    own = draft_node_queries.shape[0]
    rows = -(-own // 8) * 8
    if rows != own:
        pad = ((0, rows - own), (0, 0))
        draft_node_queries = jnp.pad(draft_node_queries, pad)
        draft_node_keys = jnp.pad(draft_node_keys, pad)
        draft_node_values = jnp.pad(draft_node_values, pad)
    cached, cache_width = paged_key_cache.shape
    picked = accepted_path.shape[0]
    q_width = QUERY_HEADS * HEAD_WIDTH
    vmem = pl.BlockSpec(memory_space=pltpu.VMEM)
    anywhere = pl.BlockSpec(memory_space=pltpu.HBM)
    shapes = (
        jax.ShapeDtypeStruct((rows, q_width), jnp.bfloat16),
        jax.ShapeDtypeStruct((picked, out_weight.shape[0]), jnp.bfloat16),
    )
    held = pl.pallas_call(
        functools.partial(kernel, n, own, parents.shape[0]),
        out_shape=tuple(pltpu.VMEM(shape.shape, shape.dtype) for shape in shapes),
        in_specs=[anywhere] * 9,
        out_specs=(vmem, vmem),
        scratch_shapes=[
            pltpu.SMEM(context_length.shape, jnp.int32),
            pltpu.SMEM(parents.shape, jnp.int32),
            pltpu.SMEM(accepted_path.shape, jnp.int32),
            pltpu.VMEM((rows, cache_width), jnp.bfloat16),
            pltpu.VMEM((rows, cache_width), jnp.bfloat16),
            pltpu.VMEM((n, rows, q_width), jnp.bfloat16),
            pltpu.VMEM((cached, cache_width), jnp.bfloat16),
            pltpu.VMEM((cached, cache_width), jnp.bfloat16),
            pltpu.VMEM(out_weight.shape, jnp.bfloat16),
            pltpu.VMEM((KEY_VALUE_HEADS, cached + TILE, LANES), jnp.bfloat16),
            pltpu.VMEM((KEY_VALUE_HEADS, HALF + 16, cached + LANES), jnp.bfloat16),
            pltpu.VMEM((CHUNKS, n, DEPTH, LANES), jnp.bfloat16),
            pltpu.VMEM((CHUNKS, n, DEPTH, LANES), jnp.bfloat16),
            pltpu.VMEM((CHUNKS, DEPTH, LANES), jnp.bfloat16),
            pltpu.VMEM((CHUNKS, n, DEPTH, LANES), jnp.bfloat16),
            pltpu.VMEM((2 * n * HALF, LANES), jnp.bfloat16),
            pltpu.VMEM((picked, out_weight.shape[0]), jnp.float32),
            pltpu.SemaphoreType.DMA((9,)),
            pltpu.SemaphoreType.DMA((CHUNKS,)),
            pltpu.SemaphoreType.DMA((CHUNKS,)),
            pltpu.SemaphoreType.DMA((CHUNKS,)),
            pltpu.SemaphoreType.DMA((3,)),
        ],
        compiler_params=pltpu.CompilerParams(
            collective_id=0, has_side_effects=True, vmem_limit_bytes=56 * 1024 * 1024
        ),
        name="verify_tree",
    )(
        context_length, parents, accepted_path,
        draft_node_queries, draft_node_keys, draft_node_values,
        paged_key_cache, paged_value_cache, out_weight,
    )
    attention, path_output = pl.pallas_call(
        write_out,
        out_shape=shapes,
        in_specs=(vmem, vmem),
        out_specs=(anywhere, anywhere),
        scratch_shapes=[pltpu.SemaphoreType.DMA((2,))],
        compiler_params=pltpu.CompilerParams(vmem_limit_bytes=1024 * 1024),
        name="write_out",
    )(*held)
    return attention[:own], path_output


def solution(mesh):
    in_specs = (
        P(("req", "blk"), None),
        P(("req", "blk"), None),
        P(("req", "blk"), None),
        P(("req", "blk"), None),
        P(("req", "blk"), None),
        P("req"),
        P("req"),
        P("req"),
        P("blk", None),
    )
    out_specs = (P(("req", "blk"), None), P("req", "blk"))
    return jax.shard_map(
        functools.partial(local, mesh.shape["blk"]),
        mesh=mesh, in_specs=in_specs, out_specs=out_specs, check_vma=False,
    )
```
